32 devices in a mesh: dp: 8 (over y, x, core), tensor: 4 (over z).
Axes of the slice: x: 2, y: 2, z: 4, core: 2. Of those that a mesh axis runs over, the one named last changes fastest.
Arguments:
- grad_tokens: bfloat16 [1536, 2048], P('dp', 'tensor'), may hold values from -6 to 6
- hidden_input: bfloat16 [2048, 5120], P('dp', 'tensor'), may hold values from -6 to 6
- output_weight: bfloat16 [5120, 2048], P(None, 'tensor'), may hold values from -0.078125 to 0.078125
- image_tokens: int32 [8, 8], replicated, may hold values from 0 to 192, as said below
- moved_images: int32 [8], replicated, may hold values from 0 to 7, as said below
Outputs:
- input_grad: bfloat16 [2048, 5120], P('dp', 'tensor')
- weight_grad: float32 [5120, 2048], P('dp', 'tensor')
- bias_grad: float32 [2048], P('tensor')
The draws below stay inside these ranges and needn't reach their ends.
Inputs may be any that keep to these rules, and one draw needn't show every extreme that they name: `image_tokens`: row s lists the merged tokens of sample s's images in order: 1 to 8 positive entries, then zeros; each row sums to 192. `moved_images`: entry s is less than the number of images of sample s; those trailing images hold at most 64 merged tokens together, exactly 64 for some sample in every draw. They are encoded by owner s + 1 (owner 0 after the last).
All inputs are finite; a program needn't handle non-finite values.
Results may differ from the reference program's by a relative error of at most 0.014.
Values may be sent and summed in bfloat16 or wider, within the bound.
A program may use at most 64 MiB of HBM per device.

```python
import jax
import jax.numpy as jnp
from jax import lax

HID = 5120
OUT = 2048
IMAGES = 8
TOK_DEV = 192
MOVE_CAP = 64
ROWS = 256
SAMPLES = 8
TOKENS = 1536
BUF = 2048
HPAD = 5120
N_TENSOR = 4


def plan_images(key):
    base = jax.random.fold_in(key, 1234)
    key_count, key_cut, key_high, key_move, key_pick = jax.random.split(base, 5)
    count_images = jax.random.randint(key_count, (SAMPLES,), 1, IMAGES + 1)
    picked = jax.random.randint(key_pick, (), 0, SAMPLES)
    sample_ids = jnp.arange(SAMPLES)
    single = sample_ids == picked
    chosen = sample_ids == (picked + 1) % SAMPLES
    count_images = jnp.where(single, 1, count_images)
    count_images = jnp.where(chosen, IMAGES, count_images)
    free_cuts = jax.vmap(lambda subkey: jax.random.permutation(subkey, TOK_DEV - 1)[:IMAGES - 1] + 1)(jax.random.split(key_cut, SAMPLES))
    high_cuts = jax.random.permutation(key_high, MOVE_CAP - 1)[:IMAGES - 2] + 1 + TOK_DEV - MOVE_CAP
    chosen_cuts = jnp.concatenate([jnp.full((1,), TOK_DEV - MOVE_CAP, high_cuts.dtype), high_cuts])
    slot_ids = jnp.arange(IMAGES - 1)[None, :]
    cuts = jnp.where(chosen[:, None], chosen_cuts[None, :], free_cuts)
    cuts = jnp.where(slot_ids < count_images[:, None] - 1, cuts, TOK_DEV)
    cuts = jnp.sort(cuts, axis=1).astype(jnp.int32)
    bounds = jnp.concatenate([jnp.zeros((SAMPLES, 1), jnp.int32), cuts, jnp.full((SAMPLES, 1), TOK_DEV, jnp.int32)], axis=1)
    sizes = bounds[:, 1:] - bounds[:, :-1]
    trailing = jnp.arange(IMAGES)[None, :]
    start_index = jnp.clip(count_images[:, None] - trailing, 0, IMAGES)
    starts = jnp.take_along_axis(bounds, start_index, axis=1)
    fitting = (TOK_DEV - starts <= MOVE_CAP) & (trailing < count_images[:, None])
    wanted = jax.random.randint(key_move, (SAMPLES,), 0, IMAGES)
    allowed = fitting & (trailing <= wanted[:, None])
    moved = jnp.max(jnp.where(allowed, trailing, 0), axis=1)
    moved = jnp.where(chosen, IMAGES - 1, moved)
    return (sizes.astype(jnp.int32), moved.astype(jnp.int32))


def draw_image_tokens(key, part):
    return plan_images(key)[0]


def draw_moved_images(key, part):
    return plan_images(key)[1]


def raised(drawn, own_key, source, target, shards_of, factor):
    owner, partner = [(jnp.arange(drawn.shape[axis_at]) // (drawn.shape[axis_at] // shards_of)).reshape([-1 if axis == axis_at else 1 for axis in range(drawn.ndim)]) for axis_at in (source, target)]
    chosen = jax.random.permutation(own_key, shards_of)[partner]
    strong = (owner == chosen) | (owner == (partner + shards_of // 2) % shards_of)
    return jnp.where(strong, factor * drawn, drawn)


def block_scale(rng, extent, cuts, least, high):
    level, own = 1.0, jax.random.fold_in(rng, 6)
    for dim, blocks in cuts:
        heights = jnp.exp(jax.random.uniform(jax.random.fold_in(own, dim), (blocks,), jnp.float32, least / len(cuts), high / len(cuts)))
        level = level * jnp.repeat(heights, extent[dim] // blocks).reshape([-1 if axis == dim else 1 for axis in range(len(extent))])
    return level


def bell_draw(rng, shape, spread, bound, shards=(), kind=jnp.bfloat16):
    result = spread * jax.random.normal(rng, shape, jnp.float32)
    if shards:
        result = result * block_scale(rng, shape, shards, -0.22, 0.18)
    return jnp.clip(result, -bound, bound).astype(kind)


def gaussian_with(own_key, dims, scale, limit, pieces, heavy, held_as=jnp.bfloat16):
    entries = scale * jax.random.normal(own_key, dims, jnp.float32)
    if pieces:
        entries = entries * block_scale(own_key, dims, pieces, -0.22, 0.18)
    return jnp.clip(raised(entries, jax.random.fold_in(own_key, 3), *heavy), -limit, limit).astype(held_as)


def setup_inputs(seed: int = 0) -> dict:
    keys = jax.random.split(jax.random.key(seed), 6)
    grad_tokens = bell_draw(keys[0], (TOKENS, OUT), 1.0, 6.0, ((0, 8), (1, 4)))
    hidden_input = gaussian_with(keys[1], (BUF, HID), 1.0, 6.0, ((0, 8), (1, 4)), (0, 1, 8, 2.0))
    output_weight = bell_draw(keys[2], (HID, OUT), HID ** -0.5, 0.078125, ((1, 4),))
    image_tokens = draw_image_tokens(jax.random.fold_in(keys[5], 71), 0)
    moved_images = draw_moved_images(jax.random.fold_in(keys[5], 71), 0)
    return {"grad_tokens": grad_tokens, "hidden_input": hidden_input, "output_weight": output_weight, "image_tokens": image_tokens, "moved_images": moved_images}


root_half = 0.7071067811865476
inv_root_tau = 0.3989422804014327


def gelu_parts(values):
    normal_cdf = 0.5 * (1.0 + jax.scipy.special.erf(values * root_half))
    density = jnp.exp(-0.5 * values * values) * inv_root_tau
    return values * normal_cdf, normal_cdf + values * density


def kept_lengths(image_tokens, moved_images):
    present = jnp.sum((image_tokens > 0).astype(jnp.int32), axis=1)
    slot_ids = jnp.arange(image_tokens.shape[1], dtype=jnp.int32)
    kept_mask = slot_ids[None, :] < (present - moved_images)[:, None]
    return jnp.sum(jnp.where(kept_mask, image_tokens, 0), axis=1).astype(jnp.int32)


def reference(grad_tokens, hidden_input, output_weight, image_tokens, moved_images):
    keep_len = kept_lengths(image_tokens, moved_images)
    grad_blocks = grad_tokens.reshape(SAMPLES, TOK_DEV, OUT)
    positions = jnp.arange(TOK_DEV, dtype=jnp.int32)
    zero_value = jnp.zeros((), jnp.bfloat16)
    kept_rows = jnp.where(positions[None, :, None] < keep_len[:, None, None], grad_blocks, zero_value)
    moving = jnp.where(positions[None, TOK_DEV - MOVE_CAP:, None] >= keep_len[:, None, None],
                       grad_blocks[:, TOK_DEV - MOVE_CAP:], zero_value)
    buffers = jnp.concatenate([kept_rows, jnp.roll(moving, 1, axis=0)], axis=1)
    bias_grad = jnp.sum(grad_tokens.astype(jnp.float32), axis=0)
    inputs = hidden_input.reshape(SAMPLES, ROWS, HID)
    column_width = OUT // N_TENSOR

    def one_owner(running, owner_data):
        grad_rows, input_rows = owner_data
        grad_hidden = jnp.zeros((ROWS, HID), jnp.float32)
        for tensor_block in range(N_TENSOR):
            low = tensor_block * column_width
            partial_value = lax.dot_general(grad_rows[:, low:low + column_width], output_weight[:, low:low + column_width],
                                      (((1,), (1,)), ((), ())), preferred_element_type=jnp.float32)
            rounded = lax.optimization_barrier(partial_value.astype(jnp.bfloat16))
            grad_hidden = grad_hidden + rounded.astype(jnp.float32)
        activation, slopes = gelu_parts(input_rows.astype(jnp.float32))
        activation = activation.astype(jnp.bfloat16)
        input_grad = (grad_hidden * slopes).astype(jnp.bfloat16)
        running = running + lax.dot_general(activation, grad_rows, (((0,), (0,)), ((), ())),
                                            preferred_element_type=jnp.float32)
        return running, input_grad

    weight_sum, input_grads = lax.scan(one_owner, jnp.zeros((HID, OUT), jnp.float32), (buffers, inputs))
    weight_grad = jnp.concatenate([weight_sum, jnp.zeros((HPAD - HID, OUT), jnp.float32)], axis=0)
    return input_grads.reshape(BUF, HID), weight_grad, bias_grad
```

```python
import functools

import jax
import jax.numpy as jnp
from jax import lax
from jax.experimental import pallas as pl
from jax.experimental.pallas import tpu as pltpu
from jax.sharding import PartitionSpec as P

root_half = 0.7071067811865476
inv_root_tau = 0.3989422804014327
MESH = pl.DeviceIdType.MESH
F32 = jnp.float32
BF16 = jnp.bfloat16


def from_behind(value, axis, steps):
    count = lax.axis_size(axis)
    pairs = [(source, (source + steps) % count) for source in range(count)]
    return lax.ppermute(value, axis, pairs)


def gelu_parts(values):
    normal_cdf = 0.5 * (1.0 + lax.erf(values * root_half))
    density = jnp.exp(-0.5 * values * values) * inv_root_tau
    return (values * normal_cdf, normal_cdf + values * density)


def kept_lengths(image_tokens, moved_images):
    present = jnp.sum((image_tokens > 0).astype(jnp.int32), axis=1)
    slot_ids = jnp.arange(image_tokens.shape[1], dtype=jnp.int32)
    kept_mask = slot_ids[None, :] < (present - moved_images)[:, None]
    return jnp.sum(jnp.where(kept_mask, image_tokens, 0), axis=1)


def per_device_any(grad_tokens, hidden_input, output_weight, image_tokens, moved_images):
    dp_count = lax.axis_size("dp")
    dp_index = lax.axis_index("dp")
    tok_rows = grad_tokens.shape[0]
    buffer_rows = hidden_input.shape[0]
    tail_count = buffer_rows - tok_rows
    keep_len = kept_lengths(image_tokens, moved_images)
    own_keep = jnp.sum(jnp.where(jnp.arange(dp_count, dtype=jnp.int32) == dp_index, keep_len, 0))
    positions = jnp.arange(tok_rows, dtype=jnp.int32)[:, None]
    zero_value = jnp.zeros((), BF16)
    kept_rows = jnp.where(positions < own_keep, grad_tokens, zero_value)
    moving = jnp.where(
        positions[tok_rows - tail_count :] >= own_keep,
        grad_tokens[tok_rows - tail_count :],
        zero_value,
    )
    arrived = from_behind(moving, "dp", 1)
    grad_rows = jnp.concatenate([kept_rows, arrived], axis=0)
    bias_grad = lax.psum(jnp.sum(grad_tokens.astype(F32), axis=0), "dp")
    activation, slopes = gelu_parts(hidden_input.astype(F32))
    partials = lax.dot_general(
        grad_rows, output_weight, (((1,), (1,)), ((), ())), preferred_element_type=F32
    )
    grad_hidden = lax.psum_scatter(
        partials.astype(BF16), "tensor", scatter_dimension=1, tiled=True
    ).astype(F32)
    input_grad = (grad_hidden * slopes).astype(BF16)
    full_act = lax.all_gather(activation.astype(BF16), "tensor", axis=1, tiled=True)
    hidden_width = full_act.shape[1]
    rows_each = (hidden_width + 8 * dp_count - 1) // (8 * dp_count) * 8
    padded = jnp.pad(full_act, ((0, 0), (0, rows_each * dp_count - hidden_width)))
    weight_grad = lax.psum_scatter(
        lax.dot_general(
            padded, grad_rows, (((0,), (0,)), ((), ())), preferred_element_type=F32
        ),
        "dp",
        scatter_dimension=0,
        tiled=True,
    )
    return (input_grad, weight_grad, bias_grad)


def kernel(
    n, dpn,
    g_ref, x_ref, w_hbm, it_ref, mv_ref,
    xg_ref, wg_ref, bg_ref,
    w_ref, raw, tail, act, act_other, slope, grad, part, sbuf, up_in, dn_in, wsend, wrecv, wmid, bias,
    w_sem, core_s, core_r, act_s, act_r, tail_s, tail_r,
    up_s, up_r, dn_s, dn_r, pl_s, pl_r, mid_r, bi_s, bi_r,
):
    dp = lax.axis_index("dp")
    z = lax.axis_index("tensor")
    core = lax.rem(dp, 2)
    chip = lax.div(dp, 2)
    partner = dp + 1 - 2 * core
    chips = dpn // 2
    tok = g_ref.shape[0]
    rows = x_ref.shape[0]
    width = x_ref.shape[1]
    half = width // 2
    tails = rows - tok

    wcopy = pltpu.make_async_copy(w_hbm, w_ref, w_sem)
    wcopy.start()

    barrier = pltpu.get_barrier_semaphore()
    for k in range(1, dpn):
        pl.semaphore_signal(barrier, inc=1, device_id=(lax.rem(dp + k, dpn), z), device_id_type=MESH)

    @pl.when(z > 0)
    def _():
        pl.semaphore_signal(barrier, inc=1, device_id=(dp, z - 1), device_id_type=MESH)

    @pl.when(z < n - 1)
    def _():
        pl.semaphore_signal(barrier, inc=1, device_id=(dp, z + 1), device_id_type=MESH)

    pl.semaphore_wait(barrier, dpn - 1 + jnp.where(z > 0, 1, 0) + jnp.where(z < n - 1, 1, 0))

    def remote(src, dst, ss, rs, d, t):
        return pltpu.make_async_remote_copy(
            src_ref=src, dst_ref=dst, send_sem=ss, recv_sem=rs, device_id=(d, t), device_id_type=MESH
        )

    lane = 128
    nk = half // lane
    ptile = width // nk

    raw_copy = remote(g_ref, raw, core_s, core_r, partner, z)
    tail_src = g_ref.at[pl.ds(tok - tails, tails)]
    tail_copies = [
        remote(tail_src, tail, tail_s.at[k], tail_r, lax.rem(dp + 1 + k, dpn), z) for k in range(2)
    ]

    def act_copy(k):
        return remote(act_other.at[k], act.at[z, k, core], act_s.at[k], act_r.at[k], partner, z)

    step_rows = 64

    def gelu_tile(which, k, to_other):
        cols = pl.ds(pl.multiple_of(which * half + k * lane, lane), lane)

        def body(i, carry):
            rs = pl.ds(pl.multiple_of(i * step_rows, step_rows), step_rows)
            a, s = gelu_parts(x_ref[rs, cols].astype(F32))
            slope[rs, cols] = s
            if to_other:
                act_other[k, rs, :] = a.astype(BF16)
            else:
                act[z, k, core, rs, :] = a.astype(BF16)
            return carry

        lax.fori_loop(0, rows // step_rows, body, 0)

    def up_ag(h, k, r):
        return remote(act.at[h, k], act.at[h, k], up_s.at[r, k], up_r.at[r, k], dp, z + 1)

    def dn_ag(h, k, r):
        return remote(act.at[h, k], act.at[h, k], dn_s.at[r, k], dn_r.at[r, k], dp, z - 1)

    def up_rs(h, k, r):
        return remote(sbuf.at[h, k], up_in.at[h, k], up_s.at[r, k], up_r.at[r, k], dp, z + 1)

    def dn_rs(h, k, r):
        return remote(sbuf.at[h, k], dn_in.at[h, k], dn_s.at[r, k], dn_r.at[r, k], dp, z - 1)

    def send_own(k):
        act_copy(k).wait_recv()

        @pl.when(z < n - 1)
        def _():
            up_ag(z, k, 0).start()

        @pl.when(z > 0)
        def _():
            dn_ag(z, k, 0).start()

    for k in range(nk):
        gelu_tile(1 - core, k, True)
        act_copy(k).start()
        if k == 0:
            raw_copy.start()

            @pl.when(core == 1)
            def _():
                for c in tail_copies:
                    c.start()

        gelu_tile(core, k, False)
        if k > 0:
            send_own(k - 1)
    send_own(nk - 1)

    raw_copy.wait_recv()
    chip_sum = jnp.sum(g_ref[...].astype(F32), axis=0, keepdims=True) + jnp.sum(
        raw[...].astype(F32), axis=0, keepdims=True
    )
    bias[chip] = jnp.broadcast_to(chip_sum, bias.shape[1:])

    def keep_of(s):
        images = it_ref[pl.ds(s, 1), :].astype(F32)
        present = jnp.sum(jnp.where(images > 0, 1.0, 0.0), axis=1, keepdims=True)
        ids = lax.broadcasted_iota(jnp.int32, images.shape, 1).astype(F32)
        kept = jnp.where(ids < present - mv_ref[s].astype(F32), images, 0.0)
        return jnp.sum(kept, axis=1, keepdims=True)

    place = lax.broadcasted_iota(jnp.int32, (tok, g_ref.shape[1]), 0).astype(F32)
    zero = jnp.zeros((), F32)

    def masked_own(block, s):
        return jnp.where(place < keep_of(s), block.astype(F32), zero).astype(BF16)

    def masked_tail(block, s):
        return jnp.where(place[tok - tails :] >= keep_of(s), block.astype(F32), zero).astype(BF16)

    grad[core, 0:tok, :] = masked_own(g_ref[...], dp)
    grad[1 - core, 0:tok, :] = masked_own(raw[...], partner)
    first = 2 * chip

    @pl.when(core == 0)
    def _():
        grad[1, tok:rows, :] = masked_tail(g_ref[pl.ds(tok - tails, tails), :], first)

    @pl.when(core == 1)
    def _():
        grad[1, tok:rows, :] = masked_tail(raw[pl.ds(tok - tails, tails), :], first)

    tail_copies[0].wait_recv()
    grad[0, tok:rows, :] = masked_tail(tail[...], lax.rem(first + dpn - 1, dpn))

    def bias_copy(k):
        return remote(
            bias.at[chip], bias.at[chip], bi_s.at[k], bi_r.at[chip], lax.rem(dp + 2 * k, dpn), z
        )

    for k in range(1, chips):
        bias_copy(k).start()

    wcopy.wait()

    def all_h(i, carry):
        h = lax.div(i, nk)
        k = lax.rem(i, nk)
        at = pl.ds(pl.multiple_of(i * ptile, ptile), ptile)
        part[h, k] = lax.dot_general(
            grad[core], w_ref[at, :], (((1,), (1,)), ((), ())), preferred_element_type=F32
        )
        return carry

    lax.fori_loop(0, n * nk, all_h, 0)

    @pl.when(z == 0)
    def _():
        for r in range(1, n):
            for k in range(nk):
                sbuf[n - r, k] = part[n - r, k].astype(BF16)
                up_rs(n - r, k, r).start()

    @pl.when(z == n - 1)
    def _():
        for r in range(1, n):
            for k in range(nk):
                sbuf[r - 1, k] = part[r - 1, k].astype(BF16)
                dn_rs(r - 1, k, r).start()

    piece = lane // 2

    def relation(h):
        return jnp.where(lax.rem(chip, 2) != lax.rem(h, 2), 1, 0) + jnp.where(
            lax.div(chip, 2) != lax.div(h, 2), 2, 0
        )

    along_x = chip + 1 - 2 * lax.rem(chip, 2)
    along_y = lax.rem(chip + 2, chips)

    def owner_copy(h, k, j):
        role = relation(h) - 1
        return remote(
            wsend.at[h, k, j], wrecv.at[role, k, j], pl_s.at[h, k, j], pl_r.at[role, k, j], h * 2 + core, z
        )

    def corner_copy(h, k, j):
        through = along_x if j == 0 else along_y
        return remote(
            wsend.at[h, k, j], wmid.at[1 - j, k], pl_s.at[h, k, j], mid_r.at[1 - j, k], through * 2 + core, z
        )

    def merge(h, k):
        rel = relation(h)
        for role in (1, 2):
            late = 1 if role == 1 else 0

            @pl.when(rel == role)
            def _():
                corner_copy(h, k, late).wait_recv()
                wsend[h, k, late] = (
                    wsend[h, k, late].astype(F32) + wmid[role - 1, k].astype(F32)
                ).astype(BF16)
                owner_copy(h, k, late).start()

    def weight_tile(h, k):
        acc = lax.dot_general(
            act[h, k, 0], grad[0], (((0,), (0,)), ((), ())), preferred_element_type=F32
        ) + lax.dot_general(
            act[h, k, 1], grad[1], (((0,), (0,)), ((), ())), preferred_element_type=F32
        )
        rel = relation(h)

        @pl.when(rel == 0)
        def _():
            wg_ref[k * lane : (k + 1) * lane, :] = acc

        @pl.when(rel != 0)
        def _():
            for j in range(2):
                wsend[h, k, j] = acc[j * piece : (j + 1) * piece].astype(BF16)

        @pl.when(rel == 1)
        def _():
            owner_copy(h, k, 0).start()

        @pl.when(rel == 2)
        def _():
            owner_copy(h, k, 1).start()

        @pl.when(rel == 3)
        def _():
            for j in range(2):
                corner_copy(h, k, j).start()

    for k in range(nk):
        weight_tile(z, k)

    def merge_round(r, k):
        if r == 0:
            merge(z, k)
        else:

            @pl.when(z >= r)
            def _():
                merge(z - r, k)

            @pl.when(z + r <= n - 1)
            def _():
                merge(z + r, k)

    for r in range(1, n):
        for k in range(nk):

            @pl.when(z >= r)
            def _():
                up_ag(z - r, k, r - 1).wait_recv()

                @pl.when(z < n - 1)
                def _():
                    up_ag(z - r, k, r).start()

            @pl.when(z + r <= n - 1)
            def _():
                dn_ag(z + r, k, r - 1).wait_recv()

                @pl.when(z > 0)
                def _():
                    dn_ag(z + r, k, r).start()

            @pl.when((z > 0) & (z < r))
            def _():
                h = n + z - r
                up_rs(h, k, r - 1).wait_recv()
                sbuf[h, k] = (part[h, k] + up_in[h, k].astype(F32)).astype(BF16)
                up_rs(h, k, r).start()

            @pl.when((z < n - 1) & (z + r > n - 1))
            def _():
                h = z + r - n
                dn_rs(h, k, r - 1).wait_recv()
                sbuf[h, k] = (part[h, k] + dn_in[h, k].astype(F32)).astype(BF16)
                dn_rs(h, k, r).start()

            @pl.when(z >= r)
            def _():
                weight_tile(z - r, k)

            @pl.when(z + r <= n - 1)
            def _():
                weight_tile(z + r, k)

            merge_round(r - 1, k)
            if r == n - 1 and k >= 2:
                merge_round(r, k - 2)
    for k in range(max(nk - 2, 0), nk):
        merge_round(n - 1, k)

    for k in range(1, chips):
        source = lax.rem(chip + k, chips)
        remote(
            bias.at[source], bias.at[source], bi_s.at[k], bi_r.at[source], lax.rem(dp + 2 * k, dpn), z
        ).wait_recv()
    total = bias[0]
    for k in range(1, chips):
        total = total + bias[k]
    bg_ref[...] = total[0]

    for k in range(nk):
        for j in range(2):
            rs = slice(k * lane + j * piece, k * lane + (j + 1) * piece)
            acc = wg_ref[rs, :]
            for role in range(2):
                remote(
                    wsend.at[along_x, k, j], wrecv.at[role, k, j], pl_s.at[0, k, j], pl_r.at[role, k, j],
                    partner, z,
                ).wait_recv()
                acc = acc + wrecv[role, k, j].astype(F32)
            wg_ref[rs, :] = acc

    for k in range(nk):

        @pl.when(z > 0)
        def _():
            up_rs(z, k, n - 1).wait_recv()
            part[z, k] += up_in[z, k].astype(F32)

        @pl.when(z < n - 1)
        def _():
            dn_rs(z, k, n - 1).wait_recv()
            part[z, k] += dn_in[z, k].astype(F32)

        at = slice(k * ptile, (k + 1) * ptile)
        xg_ref[:, at] = (part[z, k] * slope[:, at]).astype(BF16)

    raw_copy.wait_send()

    @pl.when(core == 1)
    def _():
        for c in tail_copies:
            c.wait_send()

    for c in range(1, chips):
        bias_copy(c).wait_send()
        h = lax.rem(chip + c, chips)
        for k in range(nk):
            for j in range(2):
                remote(
                    wsend.at[h, k, j], wrecv.at[0, k, j], pl_s.at[h, k, j], pl_r.at[0, k, j], partner, z
                ).wait_send()
    for k in range(nk):
        act_copy(k).wait_send()
        for r in range(n):

            @pl.when(z < n - 1)
            def _():
                up_rs(0, k, r).wait_send()

            @pl.when(z > 0)
            def _():
                dn_rs(0, k, r).wait_send()


def per_device_fast(n, dpn, grad_tokens, hidden_input, output_weight, image_tokens, moved_images):
    tok, cols = grad_tokens.shape
    rows, width = hidden_input.shape
    half = width // 2
    chips = dpn // 2
    lane = 128
    nk = half // lane
    ptile = width // nk
    dma = pltpu.SemaphoreType.DMA
    vmem = pl.BlockSpec(memory_space=pltpu.VMEM)
    return pl.pallas_call(
        functools.partial(kernel, n, dpn),
        out_shape=(
            jax.ShapeDtypeStruct((rows, width), BF16),
            jax.ShapeDtypeStruct((half, cols), F32),
            jax.ShapeDtypeStruct((cols,), F32),
        ),
        in_specs=[
            vmem, vmem, pl.BlockSpec(memory_space=pl.ANY), vmem, pl.BlockSpec(memory_space=pltpu.SMEM),
        ],
        out_specs=(vmem, vmem, vmem),
        scratch_shapes=[
            pltpu.VMEM(output_weight.shape, BF16),
            pltpu.VMEM((tok, cols), BF16),
            pltpu.VMEM((rows - tok, cols), BF16),
            pltpu.VMEM((n, nk, 2, rows, lane), BF16),
            pltpu.VMEM((nk, rows, lane), BF16),
            pltpu.VMEM((rows, width), F32),
            pltpu.VMEM((2, rows, cols), BF16),
            pltpu.VMEM((n, nk, rows, ptile), F32),
            pltpu.VMEM((n, nk, rows, ptile), BF16),
            pltpu.VMEM((n, nk, rows, ptile), BF16),
            pltpu.VMEM((n, nk, rows, ptile), BF16),
            pltpu.VMEM((chips, nk, 2, lane // 2, cols), BF16),
            pltpu.VMEM((2, nk, 2, lane // 2, cols), BF16),
            pltpu.VMEM((2, nk, lane // 2, cols), BF16),
            pltpu.VMEM((chips, 8, cols), F32),
            dma,
            dma,
            dma,
            dma((nk,)),
            dma((nk,)),
            dma((2,)),
            dma,
            dma((n, nk)),
            dma((n, nk)),
            dma((n, nk)),
            dma((n, nk)),
            dma((chips, nk, 2)),
            dma((2, nk, 2)),
            dma((2, nk)),
            dma((chips,)),
            dma((chips,)),
        ],
        compiler_params=pltpu.CompilerParams(
            collective_id=0, has_side_effects=True, vmem_limit_bytes=60 * 1024 * 1024
        ),
    )(grad_tokens, hidden_input, output_weight, image_tokens, moved_images)


def solution(mesh):
    n, dpn = mesh.shape["tensor"], mesh.shape["dp"]
    fast = dpn == 2 * n == 2 * 2 * 2
    return jax.shard_map(
        functools.partial(per_device_fast, n, dpn) if fast else per_device_any,
        mesh=mesh,
        in_specs=(P("dp", "tensor"), P("dp", "tensor"), P(None, "tensor"), P(), P()),
        out_specs=(P("dp", "tensor"), P("dp", "tensor"), P("tensor")),
        check_vma=False,
    )
```
